1024 devices in a mesh: dp: 64 (over z_lo, x), expert: 16 (over y, z_hi, core).
Axes of the slice: x: 4, y: 4, z: 32 (z_hi: 2, z_lo: 16; z = z_hi * 16 + z_lo), core: 2. Of those that a mesh axis runs over, the one named last changes fastest.
Arguments:
- out_grad: bfloat16 [1024, 3072], P('expert', 'dp'), may hold values from -6 to 6
- gate_probs: bfloat16 [1024, 2], P('expert'), may hold values from 0.049804688 to 1
- expert_ids: int32 [1024, 2], P('expert'), may hold values from 0 to 7, all different within a row; in each aligned block of 64 rows (0 to 63, 64 to 127, ...) at most 20 rows name the same one
- saved_gate: bfloat16 [16, 320, 8192], P('expert', None, 'dp'), may hold values from -8 to 8
- saved_up: bfloat16 [16, 320, 8192], P('expert', None, 'dp'), may hold values from -6 to 6
- w_gate: bfloat16 [16, 3072, 8192], P('expert', None, 'dp'), may hold values from -0.109375 to 0.109375
- w_up: bfloat16 [16, 3072, 8192], P('expert', None, 'dp'), may hold values from -0.109375 to 0.109375
- w_down: bfloat16 [16, 8192, 3072], P('expert', 'dp'), may hold values from -0.046875 to 0.046875
Outputs:
- token_grads: bfloat16 [1024, 3072], P('expert', 'dp')
The draws below stay inside these ranges and needn't reach their ends.
Inputs may be any that keep to these rules, and one draw needn't show every extreme that they name: `expert_ids`: the 2 ids of a row differ. Within the rows of one device (aligned blocks of 64 rows) no expert is named by more than 20 rows, a bound that some block reaches.
All inputs are finite; a program needn't handle non-finite values.
Results may differ from the reference program's by a relative error of at most 0.013.
Values may be sent and summed in bfloat16 or wider, within the bound.
No kernel may reach another device: no remote copies, remote signals or barrier semaphores. Data moves between devices by JAX's collectives and lax.ppermute only.
A program may use at most 32 MiB of HBM per device.

```python
import math
import jax
import jax.numpy as jnp
import numpy as np
from jax import lax

D = 3072
FF = 16384
TOP = 2
SPLIT = 2
TOK_DEV = 64
EXPERTS = 8
TOKENS = 1024
CAP = 20
SLOTS = 320
N_EXPERT = 16


def shard_levels(stream_key, shape, pieces, low, largest):
    level, own = 1.0, jax.random.fold_in(stream_key, 6)
    for dim, blocks in pieces:
        steps = jnp.exp(jax.random.uniform(jax.random.fold_in(own, dim), (blocks,), jnp.float32, low / len(pieces), largest / len(pieces)))
        level = level * jnp.repeat(steps, shape[dim] // blocks).reshape([-1 if axis == dim else 1 for axis in range(len(shape))])
    return level


def assign_block(stream_key, own, number, rows, number_of, top, most, slope):
    order = jax.random.permutation(stream_key, number_of)
    heavy_load, common = shares(number_of, rows * top, most, slope, True), shares(number_of, rows * top, most, slope, False)
    places = jnp.arange(number_of)

    def named(sizes, offset_by):
        used = int((sizes > 0).sum())
        fixed = max(1, used // 4)
        moved = fixed + (places - fixed + offset_by * (used - fixed)) % max(1, number_of - fixed)
        return jnp.zeros((number_of,), jnp.int32).at[order[jnp.where(places < fixed, places, moved)]].set(jnp.asarray(sizes, jnp.int32))

    sizes = jnp.where(number % 4 == 0, named(heavy_load, number // 4), named(common, number - number // 4 - 1))
    mixed = jax.random.permutation(jax.random.fold_in(own, 3), number_of)
    giver, sink = mixed[0:number_of // 2 * 2:2], mixed[1:number_of // 2 * 2:2]
    room = jnp.minimum(sizes[giver] - 1, most - sizes[sink]) // 2
    room = jnp.where((giver == order[0]) | (sink == order[0]) | (sizes[sink] == 0), 0, jnp.maximum(room, 0))
    moved = jax.random.randint(jax.random.fold_in(own, 4), (number_of // 2,), 0, 1 << 20) % (room + 1)
    sizes = sizes.at[giver].add(-moved).at[sink].add(moved)
    members = jnp.searchsorted(jnp.cumsum(sizes), jnp.arange(rows * top), side="right").astype(jnp.int32)
    grid = members.reshape(top, rows).T
    grid = grid[jax.random.permutation(jax.random.fold_in(own, 1), rows)]
    offset_by = jax.random.randint(jax.random.fold_in(own, 2), (rows, 1), 0, top)
    return jnp.take_along_axis(grid, (jnp.arange(top)[None, :] + offset_by) % top, axis=1)


def shares(number_of, total, most, skew, full):
    weights = [(1 << 20) // math.isqrt(standing ** skew) + 1 for standing in range(1, number_of + 1)]
    largest = most if full else min(most, max(-(-total // number_of), total * weights[0] // sum(weights)))
    least = 1 if total - largest >= number_of - 1 else 0
    counts, rest = [largest] + [least] * (number_of - 1), total - largest - least * (number_of - 1)
    while rest > 0:
        movable = [i for i in range(1, number_of) if counts[i] < largest] or [i for i in range(1, number_of) if counts[i] < most]
        pool, left = sum([weights[i] for i in movable]), rest
        for i in movable:
            addition = min(most - counts[i], max(1, left * weights[i] // pool), rest)
            counts[i] = counts[i] + addition
            rest = rest - addition
    return np.array(counts)


def centred(key, shape, scale, most, pieces=(), kind=jnp.bfloat16):
    entries = jax.random.normal(key, shape, jnp.float32) * scale
    if len(pieces) > 0:
        entries = shard_levels(key, shape, pieces, -0.22, 0.18) * entries
    return jnp.clip(entries, min=-most, max=most).astype(kind)


def setup_inputs(seed: int = 0) -> dict:
    seeds = jax.random.split(jax.random.key(seed), 9)
    out_grad = centred(seeds[0], (TOKENS, D), 1.0, 6.0, ((0, 16), (1, 64)))
    gate_probs = jnp.clip(jnp.exp(math.log(1.0) - 2.9996462 * jax.random.uniform(seeds[1], (TOKENS, TOP), jnp.float32) ** shard_levels(seeds[1], (TOKENS, TOP), ((0, 16),), -0.2, 0.2)), 0.049804688, 1.0).astype(jnp.bfloat16)
    expert_ids_keys = jax.random.split(jax.random.fold_in(seeds[2], 1), TOKENS // TOK_DEV)
    expert_ids_turns = jax.random.permutation(jax.random.fold_in(seeds[2], 3), TOKENS // TOK_DEV)
    expert_ids = jax.vmap(lambda own, number: assign_block(jax.random.fold_in(seeds[2], 2), own, number, TOK_DEV, EXPERTS, TOP, CAP, 1))(expert_ids_keys, expert_ids_turns).reshape((TOKENS, TOP))
    saved_gate = centred(seeds[3], (EXPERTS * SPLIT, SLOTS, FF // SPLIT), 1.5, 8.0, ((0, 16), (2, 64)))
    saved_up = centred(seeds[4], (EXPERTS * SPLIT, SLOTS, FF // SPLIT), 1.0, 6.0, ((0, 16), (2, 64)))
    w_gate = centred(seeds[5], (EXPERTS * SPLIT, D, FF // SPLIT), D ** -0.5, 0.109375, ((0, 16), (2, 64)))
    w_up = centred(seeds[6], (EXPERTS * SPLIT, D, FF // SPLIT), D ** -0.5, 0.109375, ((0, 16), (2, 64)))
    w_down = centred(seeds[7], (EXPERTS * SPLIT, FF // SPLIT, D), FF ** -0.5, 0.046875, ((0, 16), (1, 64)))
    return dict(out_grad=out_grad, gate_probs=gate_probs, expert_ids=expert_ids, saved_gate=saved_gate, saved_up=saved_up, w_gate=w_gate, w_up=w_up, w_down=w_down)


def slot_layout(expert_ids):
    experts_iota = jnp.arange(EXPERTS, dtype=jnp.int32)
    chosen = (expert_ids[:, :, None] == experts_iota[None, None, :]).astype(jnp.int32)
    per_token = jnp.sum(chosen, axis=1, dtype=jnp.int32)
    blocks = per_token.reshape(N_EXPERT, TOK_DEV, EXPERTS)
    ranked = (jnp.cumsum(blocks, axis=1, dtype=jnp.int32) - blocks).reshape(TOKENS, EXPERTS)
    position = jnp.sum(chosen * ranked[:, None, :], axis=2, dtype=jnp.int32)
    source = jnp.arange(TOKENS, dtype=jnp.int32) // TOK_DEV
    return (source[:, None] * CAP + position).astype(jnp.int32)


def join_parts(array):
    parts, rows, width = array.shape
    split = array.reshape(EXPERTS, SPLIT, rows, width)
    return split.transpose(0, 2, 1, 3).reshape(EXPERTS, rows, SPLIT * width)


def expert_backward(inputs):
    slot_grad, slot_prob, gate_pre, up_pre, gate_weight, up_weight, down_weight = inputs
    projected = jnp.dot(slot_grad, down_weight.T, preferred_element_type=jnp.float32)
    gate_pre = gate_pre.astype(jnp.float32)
    up_pre = up_pre.astype(jnp.float32)
    sigmoid_gate = jax.nn.sigmoid(gate_pre)
    hidden_grad = slot_prob.astype(jnp.float32)[:, None] * projected
    gate_grad = (hidden_grad * up_pre * sigmoid_gate * (1.0 + gate_pre * (1.0 - sigmoid_gate))).astype(jnp.bfloat16)
    up_grad = (hidden_grad * gate_pre * sigmoid_gate).astype(jnp.bfloat16)
    summed = jnp.dot(gate_grad, gate_weight.T, preferred_element_type=jnp.float32)
    summed = summed + jnp.dot(up_grad, up_weight.T, preferred_element_type=jnp.float32)
    return summed.astype(jnp.bfloat16)


def reference(out_grad, gate_probs, expert_ids, saved_gate, saved_up, w_gate, w_up, w_down):
    slot_ids = slot_layout(expert_ids)
    spread = jnp.broadcast_to(out_grad[:, None, :], (TOKENS, TOP, D))
    slot_grads = jnp.zeros((EXPERTS, SLOTS, D), jnp.bfloat16).at[expert_ids, slot_ids].set(spread)
    slot_probs = jnp.zeros((EXPERTS, SLOTS), jnp.bfloat16).at[expert_ids, slot_ids].set(gate_probs)
    gate_full = join_parts(saved_gate)
    up_full = join_parts(saved_up)
    gate_weights = join_parts(w_gate)
    up_weights = join_parts(w_up)
    down_weights = w_down.reshape(EXPERTS, FF, D)
    slot_back = lax.map(expert_backward, (slot_grads, slot_probs, gate_full, up_full, gate_weights, up_weights, down_weights))
    picked = slot_back[expert_ids, slot_ids].astype(jnp.float32)
    return jnp.sum(picked, axis=1).astype(jnp.bfloat16)
```

```python
import jax
import jax.numpy as jnp
from jax import lax
from jax.sharding import Mesh
from jax.sharding import PartitionSpec as P

EXPERT = ("y", "zh", "c")
DP = ("z", "x")
FAR = ("z", "y", "zh")
F32 = jnp.float32
BF16 = jnp.bfloat16


def exchange(tiles, axes):
    return lax.all_to_all(tiles, axes, split_axis=0, concat_axis=0, tiled=True)


def local(out_grad, gate_probs, expert_ids, saved_gate, saved_up, w_gate, w_up, w_down):
    nz, nx, ny, nh, nc = (lax.axis_size(a) for a in ("z", "x", "y", "zh", "c"))
    experts = ny * nh
    tokens, width = out_grad.shape
    slots = saved_gate.shape[1]
    cap = slots // (experts * nc)
    half = experts * cap
    hid = w_down.shape[1]
    chunk = cap * width
    padded = -(-chunk // 1024) * 1024

    iota = jnp.arange(experts, dtype=jnp.int32)
    chosen = (expert_ids[:, :, None] == iota[None, None, :]).astype(jnp.int32)
    per_token = jnp.sum(chosen, axis=1, dtype=jnp.int32)
    ranked = jnp.cumsum(per_token, axis=0, dtype=jnp.int32) - per_token
    position = jnp.sum(chosen * ranked[:, None, :], axis=2, dtype=jnp.int32)
    target = expert_ids * cap + position
    slot_iota = jnp.arange(half, dtype=jnp.int32)
    matches = slot_iota[:, None, None] == target[None, :, :]
    picker = jnp.any(matches, axis=2).astype(BF16)
    weighted = jnp.where(matches, gate_probs.astype(F32)[None, :, :], 0.0)
    weighted = jnp.sum(weighted, axis=2).astype(BF16)

    sent = jnp.dot(weighted, out_grad, preferred_element_type=F32).astype(BF16)
    sent = jnp.pad(sent.reshape(experts, chunk), ((0, 0), (0, padded - chunk)))
    sent = sent.reshape(experts, padded // 128, 128)
    sent = jnp.broadcast_to(sent[None], (nz, *sent.shape)).reshape(nz * experts, padded // 128, 128)
    got = exchange(sent, FAR).reshape(nz, experts, padded)
    mine = got[:, :, :chunk].reshape(nz, experts, cap, width)
    mine = mine.transpose(1, 2, 0, 3).reshape(half, nz * width)
    rows = lax.all_gather(mine, "x")
    rows = lax.all_gather(rows, "c")

    down = w_down[0].reshape(hid, nz, nx, width).transpose(2, 0, 1, 3).reshape(nx, hid, nz * width)
    gate_w = w_gate[0].reshape(nz, nx, width, hid).transpose(1, 0, 2, 3).reshape(nx, nz * width, hid)
    up_w = w_up[0].reshape(nz, nx, width, hid).transpose(1, 0, 2, 3).reshape(nx, nz * width, hid)

    def by_core(a):
        return a[0].reshape(experts, nc, cap, hid).transpose(1, 0, 2, 3).reshape(nc * half, hid)

    gate_pre = by_core(saved_gate).astype(F32)
    up_pre = by_core(saved_up).astype(F32)
    projected = sum(
        lax.dot_general(
            rows[:, k].reshape(nc * half, nz * width),
            down[k],
            (((1,), (1,)), ((), ())),
            preferred_element_type=F32,
        )
        for k in range(nx)
    )
    sig = jax.nn.sigmoid(gate_pre)
    gate_grad = (projected * up_pre * sig * (1.0 + gate_pre * (1.0 - sig))).astype(BF16)
    up_grad = (projected * gate_pre * sig).astype(BF16)
    both = jnp.concatenate([gate_grad, up_grad], axis=1)
    weights = jnp.concatenate([gate_w, up_w], axis=2)

    shares = jnp.stack(
        [
            lax.dot_general(both, weights[k], (((1,), (1,)), ((), ())), preferred_element_type=F32)
            .astype(BF16)
            .reshape(nc, half, nz * width)
            for k in range(nx)
        ],
        axis=1,
    )
    shares = jnp.sum(exchange(shares, "c").reshape(nc, nx, half, nz * width).astype(F32), axis=0)
    shares = jnp.sum(exchange(shares.astype(BF16), "x").astype(F32), axis=0).astype(BF16)
    back = shares.reshape(experts, cap, nz, width).transpose(2, 0, 1, 3)
    back = back.reshape(nz * experts, chunk)
    back = jnp.pad(back, ((0, 0), (0, padded - chunk)))
    back = exchange(back.reshape(nz * experts, padded // 128, 128), FAR)
    back = jnp.sum(back.reshape(nz, experts, padded).astype(F32), axis=0)
    back = back[:, :chunk].reshape(half, width).astype(BF16)
    return lax.dot_general(
        picker, back, (((0,), (0,)), ((), ())), preferred_element_type=F32
    ).astype(BF16)


def solution(mesh):
    split = Mesh(mesh.devices.reshape(16, 4, 4, 2, 2), ("z", "x", "y", "zh", "c"))
    return jax.shard_map(
        local,
        mesh=split,
        in_specs=(
            P(EXPERT, DP),
            P(EXPERT, None),
            P(EXPERT, None),
            P(EXPERT, None, DP),
            P(EXPERT, None, DP),
            P(EXPERT, None, DP),
            P(EXPERT, None, DP),
            P(EXPERT, DP, None),
        ),
        out_specs=P(EXPERT, DP),
        check_vma=False,
    )
```

```python
import jax
import jax.numpy as jnp
from jax import lax
from jax.sharding import Mesh
from jax.sharding import PartitionSpec as P

EXPERT = ("y", "zh", "c")
DP = ("za", "zb", "x")
FAR = ("za", "y", "zh")
F32 = jnp.float32
BF16 = jnp.bfloat16


def exchange(tiles, axes):
    return lax.all_to_all(tiles, axes, split_axis=0, concat_axis=0, tiled=True)


def swap(value):
    return lax.ppermute(value, "c", [(0, 1), (1, 0)])


def times_t(a, b):
    return lax.dot_general(a, b, (((1,), (1,)), ((), ())), preferred_element_type=F32)


def local(out_grad, gate_probs, expert_ids, saved_gate, saved_up, w_gate, w_up, w_down):
    na, nb, nx, ny, nh, nc = (lax.axis_size(a) for a in ("za", "zb", "x", "y", "zh", "c"))
    experts = ny * nh
    width = out_grad.shape[1]
    slots = saved_gate.shape[1]
    cap = slots // (experts * nc)
    half = experts * cap
    hid = w_down.shape[1]
    span = na * nb * width
    chunk = cap * width
    padded = -(-chunk // 1024) * 1024
    tile = (padded // 128, 128)
    first_core = lax.axis_index("c") == 0

    iota = jnp.arange(experts, dtype=jnp.int32)
    chosen = (expert_ids[:, :, None] == iota[None, None, :]).astype(jnp.int32)
    per_token = jnp.sum(chosen, axis=1, dtype=jnp.int32)
    ranked = jnp.cumsum(per_token, axis=0, dtype=jnp.int32) - per_token
    position = jnp.sum(chosen * ranked[:, None, :], axis=2, dtype=jnp.int32)
    target = expert_ids * cap + position
    slot_iota = jnp.arange(half, dtype=jnp.int32)
    matches = slot_iota[:, None, None] == target[None, :, :]
    picker = jnp.any(matches, axis=2).astype(BF16)
    weighted = jnp.where(matches, gate_probs.astype(F32)[None, :, :], 0.0)
    weighted = jnp.sum(weighted, axis=2).astype(BF16)

    sent = jnp.dot(weighted, out_grad, preferred_element_type=F32).astype(BF16)
    sent = jnp.pad(sent.reshape(experts, chunk), ((0, 0), (0, padded - chunk)))
    sent = sent.reshape(experts, *tile)
    sent = jnp.broadcast_to(sent[None], (na, *sent.shape)).reshape(na * experts, *tile)
    got = exchange(sent, FAR)
    got = jnp.broadcast_to(got[None], (nb, *got.shape)).reshape(nb * na * experts, *tile)
    got = exchange(got.reshape(nb, na * experts * tile[0], 128), "zb")
    got = got.reshape(nb, na, experts, padded)[..., :chunk]
    got = got.reshape(nb, na, experts, cap, width).transpose(2, 3, 1, 0, 4)
    own_rows = lax.all_gather(got.reshape(half, span), "x")
    other_rows = swap(own_rows)

    down = w_down[0].reshape(hid, na * nb, nx, width).transpose(2, 0, 1, 3).reshape(nx, hid, span)
    gate_w = w_gate[0].reshape(na * nb, nx, width, hid).transpose(1, 0, 2, 3).reshape(nx, span, hid)
    up_w = w_up[0].reshape(na * nb, nx, width, hid).transpose(1, 0, 2, 3).reshape(nx, span, hid)

    def by_core(a):
        parts = a[0].reshape(experts, nc, cap, hid).transpose(1, 0, 2, 3).reshape(nc, half, hid)
        return (
            jnp.where(first_core, parts[0], parts[1]).astype(F32),
            jnp.where(first_core, parts[1], parts[0]).astype(F32),
        )

    gates = by_core(saved_gate)
    ups = by_core(saved_up)

    def through(rows, gate_pre, up_pre):
        projected = sum(times_t(rows[k], down[k]) for k in range(nx))
        sig = jax.nn.sigmoid(gate_pre)
        gate_grad = (projected * up_pre * sig * (1.0 + gate_pre * (1.0 - sig))).astype(BF16)
        up_grad = (projected * gate_pre * sig).astype(BF16)
        return jnp.stack(
            [
                (times_t(gate_grad, gate_w[k]) + times_t(up_grad, up_w[k])).astype(BF16)
                for k in range(nx)
            ]
        )

    for_other = through(other_rows, gates[1], ups[1])
    for_own = through(own_rows, gates[0], ups[0])
    shares = (for_own.astype(F32) + swap(for_other).astype(F32)).astype(BF16)
    shares = jnp.sum(exchange(shares, "x").astype(F32), axis=0).astype(BF16)
    back = shares.reshape(experts, cap, na, nb, width).transpose(3, 2, 0, 1, 4)
    back = back.reshape(nb, na * experts, chunk)
    back = jnp.pad(back, ((0, 0), (0, 0), (0, padded - chunk)))
    back = exchange(back.reshape(nb, na * experts * tile[0], 128), "zb")
    back = jnp.sum(back.astype(F32), axis=0).astype(BF16)
    back = exchange(back.reshape(na * experts, *tile), FAR)
    back = jnp.sum(back.reshape(na, experts, padded).astype(F32), axis=0)
    back = back[:, :chunk].reshape(half, width).astype(BF16)
    return lax.dot_general(
        picker, back, (((0,), (0,)), ((), ())), preferred_element_type=F32
    ).astype(BF16)


def solution(mesh):
    split = Mesh(mesh.devices.reshape(4, 4, 4, 4, 2, 2), ("za", "zb", "x", "y", "zh", "c"))
    return jax.shard_map(
        local,
        mesh=split,
        in_specs=(
            P(EXPERT, DP),
            P(EXPERT, None),
            P(EXPERT, None),
            P(EXPERT, None, DP),
            P(EXPERT, None, DP),
            P(EXPERT, None, DP),
            P(EXPERT, None, DP),
            P(EXPERT, DP, None),
        ),
        out_specs=P(EXPERT, DP),
        check_vma=False,
    )
```

```python
import functools

import jax
import jax.numpy as jnp
from jax import lax
from jax.experimental import pallas as pl
from jax.experimental.pallas import tpu as pltpu
from jax.sharding import Mesh
from jax.sharding import PartitionSpec as P

EXPERT = ("y", "zh", "c")
DP = ("za", "zb", "x")
FAR = ("za", "y", "zh")
F32 = jnp.float32
BF16 = jnp.bfloat16


def exchange(tiles, axes):
    return lax.all_to_all(tiles, axes, split_axis=0, concat_axis=0, tiled=True)


def swap(value):
    return lax.ppermute(value, "c", [(0, 1), (1, 0)])


def times_t(a, b):
    return lax.dot_general(a, b, (((1,), (1,)), ((), ())), preferred_element_type=F32)


PARTS = 4


def counted(shape, dim):
    return lax.broadcasted_iota(jnp.int32, shape, dim)


def placing(part, width):
    feature, lane = counted((width, 128), 0), counted((width, 128), 1)
    if part < 2:
        hit = lane == feature + part * width
    elif part == 2:
        hit = (lane == feature + 2 * width) & (feature < width // 2)
    else:
        hit = (lane == feature + 2 * width - width // 2) & (feature >= width // 2)
    return hit.astype(F32).astype(BF16)


def dispatch_kernel(ids_ref, prob_ref, grad_ref, tile_ref, pick_ref):
    copies, rows, _ = tile_ref.shape
    width, tokens = grad_ref.shape
    expert = counted((rows, tokens), 0) >> 3
    row = counted((rows, tokens), 0) & 7
    first = ids_ref[0:1, :] == expert
    second = ids_ref[1:2, :] == expert
    named = first | second
    prob = prob_ref[...].astype(F32)
    weight = jnp.where(first, prob[0:1, :], 0.0) + jnp.where(second, prob[1:2, :], 0.0)
    earlier = counted((tokens, tokens), 0) < counted((tokens, tokens), 1)
    slot = jnp.dot(
        named.astype(F32).astype(BF16),
        earlier.astype(F32).astype(BF16),
        preferred_element_type=F32,
    ).astype(jnp.int32)
    grad = grad_ref[...]
    total = jnp.zeros((rows, 128), F32)
    for part in range(PARTS):
        hit = named & (slot == row + (0, 8, 16, 12)[part])
        if part == 2:
            hit = hit & (row < 4)
        if part == 3:
            hit = hit & (row >= 4)
        pick_ref[part] = hit.astype(F32).astype(BF16)
        mine = times_t(jnp.where(hit, weight, 0.0).astype(BF16), grad).astype(BF16)
        total = total + jnp.dot(mine, placing(part, width), preferred_element_type=F32)
    tile = total.astype(BF16)
    for k in range(copies):
        tile_ref[k] = tile


def unpack_kernel(width, got_ref, out_ref):
    nb, na, rows, _ = got_ref.shape
    short = rows // 2
    at, source = counted((rows, rows), 0), counted((rows, rows), 1)
    number = at & (short - 1)
    wanted = (number >> 2) * 8 + (number & 3) + jnp.where(at >= short, 4, 0)
    halves = (source == wanted).astype(F32).astype(BF16)
    whole, upper, lower = [], [], []
    for a in range(na):
        for b in range(nb):
            tile = got_ref[b, a]
            whole.append(tile[:, :width])
            upper.append(tile[:, width : 2 * width])
            rest = jnp.dot(halves, tile, preferred_element_type=F32).astype(BF16)
            lower.append(rest[:short, 2 * width : 2 * width + width // 2])
            lower.append(rest[short:, 2 * width : 2 * width + width // 2])
    out_ref[:rows, :] = jnp.concatenate(whole, axis=1)
    out_ref[rows : 2 * rows, :] = jnp.concatenate(upper, axis=1)
    out_ref[2 * rows :, :] = jnp.concatenate(lower, axis=1)


def pack_kernel(width, in_ref, out_ref):
    nb, na, rows, _ = out_ref.shape
    peers = in_ref.shape[0]
    short = rows // 2
    total = in_ref[0].astype(F32)
    for k in range(1, peers):
        total = total + in_ref[k].astype(F32)
    total = total.astype(BF16)
    at, source = counted((rows, short), 0), counted((rows, short), 1)
    wanted = (at >> 3) * 4 + (at & 3)
    low = ((source == wanted) & ((at & 7) < 4)).astype(F32).astype(BF16)
    high = ((source == wanted) & ((at & 7) >= 4)).astype(F32).astype(BF16)
    lows = jnp.dot(low, total[2 * rows :], preferred_element_type=F32).astype(BF16)
    highs = jnp.dot(high, total[2 * rows :], preferred_element_type=F32).astype(BF16)
    blank = jnp.zeros((rows, 128 - 2 * width - width // 2), BF16)
    for a in range(na):
        for b in range(nb):
            at = (a * nb + b) * width
            half = lows[:, at : at + width // 2] + highs[:, at + width // 2 : at + width]
            out_ref[b, a] = jnp.concatenate(
                [total[:rows, at : at + width], total[rows : 2 * rows, at : at + width], half, blank],
                axis=1,
            )


def final_kernel(got_ref, pick_ref, out_ref):
    width = out_ref.shape[0]
    total = got_ref[0].astype(F32)
    for k in range(1, got_ref.shape[0]):
        total = total + got_ref[k].astype(F32)
    total = total.astype(BF16)
    out = jnp.zeros(out_ref.shape, F32)
    for part in range(PARTS):
        rows = times_t(placing(part, width), total).astype(BF16)
        out = out + jnp.dot(rows, pick_ref[part], preferred_element_type=F32)
    out_ref[...] = out.astype(BF16)


def call(kernel, name, out, *args):
    shapes = [jax.ShapeDtypeStruct(s, BF16) for s in out]
    whole = pl.BlockSpec(memory_space=pltpu.VMEM)
    return pl.pallas_call(
        kernel,
        name=name,
        out_shape=shapes,
        in_specs=[whole] * len(args),
        out_specs=[whole] * len(out),
        cost_estimate=pl.CostEstimate(flops=4000000, bytes_accessed=300000, transcendentals=0),
    )(*args)


def local(out_grad, gate_probs, expert_ids, saved_gate, saved_up, w_gate, w_up, w_down):
    na, nb, nx, ny, nh, nc = (lax.axis_size(a) for a in ("za", "zb", "x", "y", "zh", "c"))
    experts = ny * nh
    tokens, width = out_grad.shape
    slots = saved_gate.shape[1]
    cap = slots // (experts * nc)
    half = experts * cap
    hid = w_down.shape[1]
    span = na * nb * width
    rows = experts * 8
    assert cap == 20 and 2 * width + width // 2 <= 128
    first_core = lax.axis_index("c") == 0

    sent, picks = call(
        dispatch_kernel,
        "dispatch",
        [(na, rows, 128), (PARTS, rows, tokens)],
        expert_ids.T,
        gate_probs.T,
        out_grad.T,
    )
    got = exchange(sent.reshape(na * experts, 8, 128), FAR)
    got = jnp.broadcast_to(got.reshape(1, na * rows, 128), (nb, na * rows, 128))
    got = exchange(got, "zb").reshape(nb, na, rows, 128)
    (got,) = call(functools.partial(unpack_kernel, width), "unpack", [(half, span)], got)
    own_rows = lax.all_gather(got, "x")
    other_rows = swap(own_rows)

    down = w_down[0].reshape(hid, na * nb, nx, width).transpose(2, 0, 1, 3).reshape(nx, hid, span)
    gate_w = w_gate[0].reshape(na * nb, nx, width, hid).transpose(1, 0, 2, 3).reshape(nx, span, hid)
    up_w = w_up[0].reshape(na * nb, nx, width, hid).transpose(1, 0, 2, 3).reshape(nx, span, hid)

    def by_core(a):
        parts = a[0].reshape(experts, nc, cap, hid)
        parts = jnp.stack(
            [
                jnp.concatenate(
                    [parts[:, k, at:to].reshape(-1, hid) for at, to in ((0, 8), (8, 16), (16, cap))]
                )
                for k in range(nc)
            ]
        )
        return (
            jnp.where(first_core, parts[0], parts[1]).astype(F32),
            jnp.where(first_core, parts[1], parts[0]).astype(F32),
        )

    gates = by_core(saved_gate)
    ups = by_core(saved_up)

    def through(rows, gate_pre, up_pre):
        projected = sum(times_t(rows[k], down[k]) for k in range(nx))
        sig = jax.nn.sigmoid(gate_pre)
        gate_grad = (projected * up_pre * sig * (1.0 + gate_pre * (1.0 - sig))).astype(BF16)
        up_grad = (projected * gate_pre * sig).astype(BF16)
        return jnp.stack(
            [
                (times_t(gate_grad, gate_w[k]) + times_t(up_grad, up_w[k])).astype(BF16)
                for k in range(nx)
            ]
        )

    for_other = through(other_rows, gates[1], ups[1])
    for_own = through(own_rows, gates[0], ups[0])
    shares = (for_own.astype(F32) + swap(for_other).astype(F32)).astype(BF16)
    shares = exchange(shares, "x")
    (back,) = call(functools.partial(pack_kernel, width), "pack", [(nb, na, rows, 128)], shares)
    back = exchange(back.reshape(nb, na * rows, 128), "zb")
    back = jnp.sum(back.astype(F32), axis=0).astype(BF16)
    back = exchange(back.reshape(na * experts, 8, 128), FAR).reshape(na, rows, 128)
    (out,) = call(final_kernel, "pick", [(width, tokens)], back, picks)
    return out.T


def solution(mesh):
    split = Mesh(mesh.devices.reshape(4, 4, 4, 4, 2, 2), ("za", "zb", "x", "y", "zh", "c"))
    return jax.shard_map(
        local,
        mesh=split,
        in_specs=(
            P(EXPERT, DP),
            P(EXPERT, None),
            P(EXPERT, None),
            P(EXPERT, None, DP),
            P(EXPERT, None, DP),
            P(EXPERT, None, DP),
            P(EXPERT, None, DP),
            P(EXPERT, DP, None),
        ),
        out_specs=P(EXPERT, DP),
        check_vma=False,
    )
```

```python
import functools

import jax
import jax.numpy as jnp
from jax import lax
from jax.experimental import pallas as pl
from jax.experimental.pallas import tpu as pltpu
from jax.sharding import Mesh
from jax.sharding import PartitionSpec as P

EXPERT = ("y", "zh", "c")
DP = ("za", "zb", "x")
FAR = ("za", "y", "zh")
F32 = jnp.float32
BF16 = jnp.bfloat16


def exchange(tiles, axes):
    return lax.all_to_all(tiles, axes, split_axis=0, concat_axis=0, tiled=True)


def swap(value):
    return lax.ppermute(value, "c", [(0, 1), (1, 0)])


def times_t(a, b):
    return lax.dot_general(a, b, (((1,), (1,)), ((), ())), preferred_element_type=F32)


PARTS = 4


def counted(shape, dim):
    return lax.broadcasted_iota(jnp.int32, shape, dim)


def placing(part, width):
    feature, lane = counted((width, 128), 0), counted((width, 128), 1)
    if part < 2:
        hit = lane == feature + part * width
    elif part == 2:
        hit = (lane == feature + 2 * width) & (feature < width // 2)
    else:
        hit = (lane == feature + 2 * width - width // 2) & (feature >= width // 2)
    return hit.astype(F32).astype(BF16)


def dispatch_kernel(ids_ref, prob_ref, grad_ref, tile_ref, pick_ref):
    copies, rows, _ = tile_ref.shape
    width, tokens = grad_ref.shape
    expert = counted((rows, tokens), 0) >> 3
    row = counted((rows, tokens), 0) & 7
    first = ids_ref[0:1, :] == expert
    second = ids_ref[1:2, :] == expert
    named = first | second
    prob = prob_ref[...].astype(F32)
    weight = jnp.where(first, prob[0:1, :], 0.0) + jnp.where(second, prob[1:2, :], 0.0)
    earlier = counted((tokens, tokens), 0) < counted((tokens, tokens), 1)
    slot = jnp.dot(
        named.astype(F32).astype(BF16),
        earlier.astype(F32).astype(BF16),
        preferred_element_type=F32,
    ).astype(jnp.int32)
    grad = grad_ref[...]
    total = jnp.zeros((rows, 128), F32)
    for part in range(PARTS):
        hit = named & (slot == row + (0, 8, 16, 12)[part])
        if part == 2:
            hit = hit & (row < 4)
        if part == 3:
            hit = hit & (row >= 4)
        pick_ref[part] = hit.astype(F32).astype(BF16)
        mine = times_t(jnp.where(hit, weight, 0.0).astype(BF16), grad).astype(BF16)
        total = total + jnp.dot(mine, placing(part, width), preferred_element_type=F32)
    tile = total.astype(BF16)
    for k in range(copies):
        tile_ref[k] = tile


def unpack_kernel(width, got_ref, out_ref):
    nb, na, rows, _ = got_ref.shape
    short = rows // 2
    at, source = counted((rows, rows), 0), counted((rows, rows), 1)
    number = at & (short - 1)
    wanted = (number >> 2) * 8 + (number & 3) + jnp.where(at >= short, 4, 0)
    halves = (source == wanted).astype(F32).astype(BF16)
    whole, upper, lower = [], [], []
    for a in range(na):
        for b in range(nb):
            tile = got_ref[b, a]
            whole.append(tile[:, :width])
            upper.append(tile[:, width : 2 * width])
            rest = jnp.dot(halves, tile, preferred_element_type=F32).astype(BF16)
            lower.append(rest[:short, 2 * width : 2 * width + width // 2])
            lower.append(rest[short:, 2 * width : 2 * width + width // 2])
    out_ref[:rows, :] = jnp.concatenate(whole, axis=1)
    out_ref[rows : 2 * rows, :] = jnp.concatenate(upper, axis=1)
    out_ref[2 * rows :, :] = jnp.concatenate(lower, axis=1)


def pack_kernel(width, in_ref, out_ref):
    nb, na, rows, _ = out_ref.shape
    peers = in_ref.shape[0]
    short = rows // 2
    total = in_ref[0].astype(F32)
    for k in range(1, peers):
        total = total + in_ref[k].astype(F32)
    total = total.astype(BF16)
    at, source = counted((rows, short), 0), counted((rows, short), 1)
    wanted = (at >> 3) * 4 + (at & 3)
    low = ((source == wanted) & ((at & 7) < 4)).astype(F32).astype(BF16)
    high = ((source == wanted) & ((at & 7) >= 4)).astype(F32).astype(BF16)
    lows = jnp.dot(low, total[2 * rows :], preferred_element_type=F32).astype(BF16)
    highs = jnp.dot(high, total[2 * rows :], preferred_element_type=F32).astype(BF16)
    blank = jnp.zeros((rows, 128 - 2 * width - width // 2), BF16)
    for a in range(na):
        for b in range(nb):
            at = (a * nb + b) * width
            half = lows[:, at : at + width // 2] + highs[:, at + width // 2 : at + width]
            out_ref[b, a] = jnp.concatenate(
                [total[:rows, at : at + width], total[rows : 2 * rows, at : at + width], half, blank],
                axis=1,
            )


def final_kernel(got_ref, pick_ref, out_ref):
    width = out_ref.shape[0]
    total = got_ref[0].astype(F32)
    for k in range(1, got_ref.shape[0]):
        total = total + got_ref[k].astype(F32)
    total = total.astype(BF16)
    out = jnp.zeros(out_ref.shape, F32)
    for part in range(PARTS):
        rows = times_t(placing(part, width), total).astype(BF16)
        out = out + jnp.dot(rows, pick_ref[part], preferred_element_type=F32)
    out_ref[...] = out.astype(BF16)


def weights_kernel(
    cap, core_ref, down_ref, gate_ref, up_ref, gates_ref, ups_ref, down_out, both_out, pre_out, turned
):
    nx, nz, width, hid = down_out.shape
    features = nx * nz * width
    for at in range(0, features, 128):
        to = min(at + 128, features)
        turned[at:to, :] = down_ref[:, at:to].T
    for z in range(nz):
        for x in range(nx):
            at = (z * nx + x) * width
            down_out[x, z] = turned[at : at + width, :]
            both_out[x, z, :, :hid] = gate_ref[at : at + width, :]
            both_out[x, z, :, hid:] = up_ref[at : at + width, :]
    slots = gates_ref.shape[0]
    half = slots // 2
    eight = half // cap * 8
    row, source = counted((half, slots), 0), counted((half, slots), 1)
    rest = row - 2 * eight
    block = jnp.where(row < 2 * eight, (row & (eight - 1)) >> 3, rest >> 2)
    slot = jnp.where(row < eight, row & 7, jnp.where(row < 2 * eight, 8 + (row & 7), 16 + (rest & 3)))
    for other in range(2):
        core = core_ref[0] if other == 0 else 1 - core_ref[0]
        picks = (source == (block * 2 + core) * cap + slot).astype(F32).astype(BF16)
        pre_out[other, 0] = jnp.dot(picks, gates_ref[...], preferred_element_type=F32).astype(BF16)
        pre_out[other, 1] = jnp.dot(picks, ups_ref[...], preferred_element_type=F32).astype(BF16)


def through_kernel(other, rows_ref, down_ref, both_ref, pre_ref, out_ref):
    nx = rows_ref.shape[0]
    projected = jnp.dot(rows_ref[0], down_ref[0], preferred_element_type=F32)
    for k in range(1, nx):
        projected = projected + jnp.dot(rows_ref[k], down_ref[k], preferred_element_type=F32)
    gate_pre = pre_ref[other, 0].astype(F32)
    up_pre = pre_ref[other, 1].astype(F32)
    sig = jax.nn.sigmoid(gate_pre)
    gate_grad = (projected * up_pre * sig * (1.0 + gate_pre * (1.0 - sig))).astype(BF16)
    up_grad = (projected * gate_pre * sig).astype(BF16)
    both = jnp.concatenate([gate_grad, up_grad], axis=1)
    for k in range(nx):
        out_ref[k] = times_t(both, both_ref[k]).astype(out_ref.dtype)


def call(kernel, name, out, *args, dtype=BF16, scratch=(), flops=4000000):
    shapes = [jax.ShapeDtypeStruct(s, dtype) for s in out]
    whole = pl.BlockSpec(memory_space=pltpu.VMEM)
    scalars = pl.BlockSpec(memory_space=pltpu.SMEM)
    return pl.pallas_call(
        kernel,
        name=name,
        out_shape=shapes,
        in_specs=[scalars if a.ndim == 1 else whole for a in args],
        out_specs=[whole] * len(out),
        scratch_shapes=scratch,
        compiler_params=pltpu.CompilerParams(vmem_limit_bytes=8 << 20),
        cost_estimate=pl.CostEstimate(flops=flops, bytes_accessed=300000, transcendentals=0),
    )(*args)


def local(out_grad, gate_probs, expert_ids, saved_gate, saved_up, w_gate, w_up, w_down):
    na, nb, nx, ny, nh, nc = (lax.axis_size(a) for a in ("za", "zb", "x", "y", "zh", "c"))
    experts = ny * nh
    tokens, width = out_grad.shape
    slots = saved_gate.shape[1]
    cap = slots // (experts * nc)
    half = experts * cap
    hid = w_down.shape[1]
    span = na * nb * width
    rows = experts * 8
    assert cap == 20 and 2 * width + width // 2 <= 128

    sent, picks = call(
        dispatch_kernel,
        "dispatch",
        [(na, rows, 128), (PARTS, rows, tokens)],
        expert_ids.T,
        gate_probs.T,
        out_grad.T,
    )
    got = exchange(sent.reshape(na * experts, 8, 128), FAR)
    got, w_down = lax.optimization_barrier((got, w_down))

    features = nx * span
    nz = na * nb
    down, both, pre = call(
        functools.partial(weights_kernel, cap),
        "weights",
        [(nx, nz, width, hid), (nx, nz, width, 2 * hid), (2, 2, half, hid)],
        lax.axis_index("c").astype(jnp.int32).reshape(1),
        w_down[0],
        w_gate[0],
        w_up[0],
        saved_gate[0],
        saved_up[0],
        scratch=[pltpu.VMEM((features, hid), BF16)],
        flops=100000000,
    )
    down = down.reshape(nx, span, hid)
    both = both.reshape(nx, span, 2 * hid)
    got = jnp.broadcast_to(got.reshape(1, na * rows, 128), (nb, na * rows, 128))
    got = exchange(got, "zb").reshape(nb, na, rows, 128)
    got, down, both, pre = lax.optimization_barrier((got, down, both, pre))
    (got,) = call(functools.partial(unpack_kernel, width), "unpack", [(half, span)], got)
    own_rows = lax.all_gather(got, "x")
    other_rows = swap(own_rows)

    def through(rows, other, dtype):
        (out,) = call(
            functools.partial(through_kernel, other),
            ("own", "other")[other],
            [(nx, half, span)],
            rows,
            down,
            both,
            pre,
            dtype=dtype,
            flops=2 * half * features * hid * 3,
        )
        return out

    for_own = through(own_rows, 0, F32)
    for_other = through(other_rows, 1, BF16)
    shares = (for_own + swap(for_other).astype(F32)).astype(BF16)
    shares = exchange(shares, "x")
    (back,) = call(functools.partial(pack_kernel, width), "pack", [(nb, na, rows, 128)], shares)
    back = exchange(back.reshape(nb, na * rows, 128), "zb")
    back = jnp.sum(back.astype(F32), axis=0).astype(BF16)
    back = exchange(back.reshape(na * experts, 8, 128), FAR).reshape(na, rows, 128)
    (out,) = call(final_kernel, "pick", [(width, tokens)], back, picks)
    return out.T


def solution(mesh):
    split = Mesh(mesh.devices.reshape(4, 4, 4, 4, 2, 2), ("za", "zb", "x", "y", "zh", "c"))
    return jax.shard_map(
        local,
        mesh=split,
        in_specs=(
            P(EXPERT, DP),
            P(EXPERT, None),
            P(EXPERT, None),
            P(EXPERT, None, DP),
            P(EXPERT, None, DP),
            P(EXPERT, None, DP),
            P(EXPERT, None, DP),
            P(EXPERT, DP, None),
        ),
        out_specs=P(EXPERT, DP),
        check_vma=False,
    )
```

```python
import functools

import jax
import jax.numpy as jnp
from jax import lax
from jax.experimental import pallas as pl
from jax.experimental.pallas import tpu as pltpu
from jax.sharding import Mesh
from jax.sharding import PartitionSpec as P

EXPERT = ("y", "zh", "c")
DP = ("za", "zb", "x")
FAR = ("za", "y", "zh")
F32 = jnp.float32
BF16 = jnp.bfloat16


def exchange(tiles, axes):
    return lax.all_to_all(tiles, axes, split_axis=0, concat_axis=0, tiled=True)


def swap(value):
    return lax.ppermute(value, "c", [(0, 1), (1, 0)])


def times_t(a, b):
    return lax.dot_general(a, b, (((1,), (1,)), ((), ())), preferred_element_type=F32)


PARTS = 4


def counted(shape, dim):
    return lax.broadcasted_iota(jnp.int32, shape, dim)


def placing(part, width):
    feature, lane = counted((width, 128), 0), counted((width, 128), 1)
    if part < 2:
        hit = lane == feature + part * width
    elif part == 2:
        hit = (lane == feature + 2 * width) & (feature < width // 2)
    else:
        hit = (lane == feature + 2 * width - width // 2) & (feature >= width // 2)
    return hit.astype(F32).astype(BF16)


def dispatch_kernel(width, in_ref, tile_ref, pick_ref):
    copies, rows, _ = tile_ref.shape
    tokens = in_ref.shape[1]
    routing = in_ref[width:, :].astype(F32)
    expert = counted((rows, tokens), 0) >> 3
    row = counted((rows, tokens), 0) & 7
    first = routing[0:1, :].astype(jnp.int32) == expert
    second = routing[1:2, :].astype(jnp.int32) == expert
    named = first | second
    weight = jnp.where(first, routing[2:3, :], 0.0) + jnp.where(second, routing[3:4, :], 0.0)
    earlier = counted((tokens, tokens), 0) < counted((tokens, tokens), 1)
    slot = jnp.dot(
        named.astype(F32).astype(BF16),
        earlier.astype(F32).astype(BF16),
        preferred_element_type=F32,
    ).astype(jnp.int32)
    grad = in_ref[:width, :]
    total = jnp.zeros((rows, 128), F32)
    for part in range(PARTS):
        hit = named & (slot == row + (0, 8, 16, 12)[part])
        if part == 2:
            hit = hit & (row < 4)
        if part == 3:
            hit = hit & (row >= 4)
        pick_ref[part] = hit.astype(F32).astype(BF16)
        mine = times_t(jnp.where(hit, weight, 0.0).astype(BF16), grad).astype(BF16)
        total = total + jnp.dot(mine, placing(part, width), preferred_element_type=F32)
    tile = total.astype(BF16)
    for k in range(copies):
        tile_ref[k] = tile


def unpack_kernel(width, got_ref, out_ref):
    nb, na, rows, _ = got_ref.shape
    short = rows // 2
    at, source = counted((rows, rows), 0), counted((rows, rows), 1)
    number = at & (short - 1)
    wanted = (number >> 2) * 8 + (number & 3) + jnp.where(at >= short, 4, 0)
    halves = (source == wanted).astype(F32).astype(BF16)
    whole, upper, lower = [], [], []
    for a in range(na):
        for b in range(nb):
            tile = got_ref[b, a]
            whole.append(tile[:, :width])
            upper.append(tile[:, width : 2 * width])
            rest = jnp.dot(halves, tile, preferred_element_type=F32).astype(BF16)
            lower.append(rest[:short, 2 * width : 2 * width + width // 2])
            lower.append(rest[short:, 2 * width : 2 * width + width // 2])
    out_ref[:rows, :] = jnp.concatenate(whole, axis=1)
    out_ref[rows : 2 * rows, :] = jnp.concatenate(upper, axis=1)
    out_ref[2 * rows :, :] = jnp.concatenate(lower, axis=1)


def pack_kernel(width, in_ref, out_ref):
    nb, na, rows, _ = out_ref.shape
    peers = in_ref.shape[0]
    short = rows // 2
    total = in_ref[0].astype(F32)
    for k in range(1, peers):
        total = total + in_ref[k].astype(F32)
    total = total.astype(BF16)
    at, source = counted((rows, short), 0), counted((rows, short), 1)
    wanted = (at >> 3) * 4 + (at & 3)
    low = ((source == wanted) & ((at & 7) < 4)).astype(F32).astype(BF16)
    high = ((source == wanted) & ((at & 7) >= 4)).astype(F32).astype(BF16)
    lows = jnp.dot(low, total[2 * rows :], preferred_element_type=F32).astype(BF16)
    highs = jnp.dot(high, total[2 * rows :], preferred_element_type=F32).astype(BF16)
    blank = jnp.zeros((rows, 128 - 2 * width - width // 2), BF16)
    for a in range(na):
        for b in range(nb):
            at = (a * nb + b) * width
            half = lows[:, at : at + width // 2] + highs[:, at + width // 2 : at + width]
            out_ref[b, a] = jnp.concatenate(
                [total[:rows, at : at + width], total[rows : 2 * rows, at : at + width], half, blank],
                axis=1,
            )


def final_kernel(got_ref, pick_ref, out_ref):
    width = out_ref.shape[0]
    total = got_ref[0].astype(F32)
    for k in range(1, got_ref.shape[0]):
        total = total + got_ref[k].astype(F32)
    total = total.astype(BF16)
    out = jnp.zeros(out_ref.shape, F32)
    for part in range(PARTS):
        rows = times_t(placing(part, width), total).astype(BF16)
        out = out + jnp.dot(rows, pick_ref[part], preferred_element_type=F32)
    out_ref[...] = out.astype(BF16)


def weights_kernel(cap, core_ref, down_ref, saved_ref, down_out, pre_out, turned):
    nx, nz, width, _ = down_out.shape
    features = nx * nz * width
    for at in range(0, features, 128):
        to = min(at + 128, features)
        turned[at:to, :] = down_ref[:, at:to].T
    for z in range(nz):
        for x in range(nx):
            at = (z * nx + x) * width
            down_out[x, z] = turned[at : at + width, :]
    slots = saved_ref.shape[1]
    half = slots // 2
    eight = half // cap * 8
    row, source = counted((half, slots), 0), counted((half, slots), 1)
    rest = row - 2 * eight
    block = jnp.where(row < 2 * eight, (row & (eight - 1)) >> 3, rest >> 2)
    slot = jnp.where(row < eight, row & 7, jnp.where(row < 2 * eight, 8 + (row & 7), 16 + (rest & 3)))
    for other in range(2):
        core = core_ref[0] if other == 0 else 1 - core_ref[0]
        picks = (source == (block * 2 + core) * cap + slot).astype(F32).astype(BF16)
        for kind in range(2):
            mine = jnp.dot(picks, saved_ref[kind], preferred_element_type=F32)
            pre_out[other, kind] = mine.astype(BF16)


def through_kernel(other, rows_ref, down_ref, both_ref, pre_ref, out_ref):
    nx = rows_ref.shape[0]
    projected = jnp.dot(rows_ref[0], down_ref[0], preferred_element_type=F32)
    for k in range(1, nx):
        projected = projected + jnp.dot(rows_ref[k], down_ref[k], preferred_element_type=F32)
    gate_pre = pre_ref[other, 0].astype(F32)
    up_pre = pre_ref[other, 1].astype(F32)
    sig = jax.nn.sigmoid(gate_pre)
    gate_grad = (projected * up_pre * sig * (1.0 + gate_pre * (1.0 - sig))).astype(BF16)
    up_grad = (projected * gate_pre * sig).astype(BF16)
    both = jnp.concatenate([gate_grad, up_grad], axis=1)
    for k in range(nx):
        weights = both_ref[:, k].reshape(out_ref.shape[2], both.shape[1])
        out_ref[k] = times_t(both, weights).astype(out_ref.dtype)


def call(kernel, name, out, *args, dtype=BF16, scratch=(), flops=4000000):
    shapes = [jax.ShapeDtypeStruct(s, dtype) for s in out]
    whole = pl.BlockSpec(memory_space=pltpu.VMEM)
    scalars = pl.BlockSpec(memory_space=pltpu.SMEM)
    return pl.pallas_call(
        kernel,
        name=name,
        out_shape=shapes,
        in_specs=[scalars if a.ndim == 1 else whole for a in args],
        out_specs=[whole] * len(out),
        scratch_shapes=scratch,
        compiler_params=pltpu.CompilerParams(vmem_limit_bytes=8 << 20),
        cost_estimate=pl.CostEstimate(flops=flops, bytes_accessed=300000, transcendentals=0),
    )(*args)


def local(out_grad, gate_probs, expert_ids, saved_gate, saved_up, w_gate, w_up, w_down):
    na, nb, nx, ny, nh, nc = (lax.axis_size(a) for a in ("za", "zb", "x", "y", "zh", "c"))
    experts = ny * nh
    tokens, width = out_grad.shape
    slots = saved_gate.shape[1]
    cap = slots // (experts * nc)
    half = experts * cap
    hid = w_down.shape[1]
    span = na * nb * width
    rows = experts * 8
    assert cap == 20 and 2 * width + width // 2 <= 128

    sent, picks = call(
        functools.partial(dispatch_kernel, width),
        "dispatch",
        [(na, rows, 128), (PARTS, rows, tokens)],
        jnp.pad(
            jnp.concatenate([out_grad.T, expert_ids.T.astype(BF16), gate_probs.T]),
            ((0, -(width + 4) % 16), (0, 0)),
        ),
    )
    got = exchange(sent.reshape(na * experts, 8, 128), FAR)
    got, w_down, w_gate, w_up, saved_gate, saved_up = lax.optimization_barrier(
        (got, w_down, w_gate, w_up, saved_gate, saved_up)
    )

    features = nx * span
    nz = na * nb
    nz = na * nb
    both = jnp.concatenate([w_gate[0], w_up[0]], axis=1).reshape(nz, nx, width, 2 * hid)
    down, pre = call(
        functools.partial(weights_kernel, cap),
        "weights",
        [(nx, nz, width, hid), (2, 2, half, hid)],
        lax.axis_index("c").astype(jnp.int32).reshape(1),
        w_down[0],
        jnp.concatenate([saved_gate, saved_up]),
        scratch=[pltpu.VMEM((features, hid), BF16)],
        flops=100000000,
    )
    down = down.reshape(nx, span, hid)
    got = jnp.broadcast_to(got.reshape(1, na * rows, 128), (nb, na * rows, 128))
    got = exchange(got, "zb").reshape(nb, na, rows, 128)
    got, down, both, pre = lax.optimization_barrier((got, down, both, pre))
    (got,) = call(functools.partial(unpack_kernel, width), "unpack", [(half, span)], got)
    own_rows = lax.all_gather(got, "x")
    other_rows = swap(own_rows)

    def through(rows, other, dtype):
        (out,) = call(
            functools.partial(through_kernel, other),
            ("own", "other")[other],
            [(nx, half, span)],
            rows,
            down,
            both,
            pre,
            dtype=dtype,
            flops=2 * half * features * hid * 3,
        )
        return out

    for_own = through(own_rows, 0, F32)
    for_other = through(other_rows, 1, BF16)
    shares = (for_own + swap(for_other).astype(F32)).astype(BF16)
    shares = exchange(shares, "x")
    (back,) = call(functools.partial(pack_kernel, width), "pack", [(nb, na, rows, 128)], shares)
    back = exchange(back.reshape(nb, na * rows, 128), "zb")
    back = jnp.sum(back.astype(F32), axis=0).astype(BF16)
    back = exchange(back.reshape(na * experts, 8, 128), FAR).reshape(na, rows, 128)
    (out,) = call(final_kernel, "pick", [(width, tokens)], back, picks)
    return out.T


def solution(mesh):
    split = Mesh(mesh.devices.reshape(4, 4, 4, 4, 2, 2), ("za", "zb", "x", "y", "zh", "c"))
    return jax.shard_map(
        local,
        mesh=split,
        in_specs=(
            P(EXPERT, DP),
            P(EXPERT, None),
            P(EXPERT, None),
            P(EXPERT, None, DP),
            P(EXPERT, None, DP),
            P(EXPERT, None, DP),
            P(EXPERT, None, DP),
            P(EXPERT, DP, None),
        ),
        out_specs=P(EXPERT, DP),
        check_vma=False,
    )
```

```python
import functools

import jax
import jax.numpy as jnp
from jax import lax
from jax.experimental import pallas as pl
from jax.experimental.pallas import tpu as pltpu
from jax.sharding import Mesh
from jax.sharding import PartitionSpec as P

EXPERT = ("y", "zh", "c")
DP = ("za", "zb", "x")
FAR = ("za", "y", "zh")
F32 = jnp.float32
BF16 = jnp.bfloat16


def exchange(tiles, axes):
    return lax.all_to_all(tiles, axes, split_axis=0, concat_axis=0, tiled=True)


def swap(value):
    return lax.ppermute(value, "c", [(0, 1), (1, 0)])


def times_t(a, b):
    return lax.dot_general(a, b, (((1,), (1,)), ((), ())), preferred_element_type=F32)


PARTS = 4


def counted(shape, dim):
    return lax.broadcasted_iota(jnp.int32, shape, dim)


def placing(part, width):
    feature, lane = counted((width, 128), 0), counted((width, 128), 1)
    if part < 2:
        hit = lane == feature + part * width
    elif part == 2:
        hit = (lane == feature + 2 * width) & (feature < width // 2)
    else:
        hit = (lane == feature + 2 * width - width // 2) & (feature >= width // 2)
    return hit.astype(F32).astype(BF16)


def dispatch_kernel(ids_ref, prob_ref, grad_ref, tile_ref, pick_ref):
    copies, rows, _ = tile_ref.shape
    width, tokens = grad_ref.shape
    expert = counted((rows, tokens), 0) >> 3
    row = counted((rows, tokens), 0) & 7
    first = ids_ref[0:1, :] == expert
    second = ids_ref[1:2, :] == expert
    named = first | second
    prob = prob_ref[...].astype(F32)
    weight = jnp.where(first, prob[0:1, :], 0.0) + jnp.where(second, prob[1:2, :], 0.0)
    earlier = counted((tokens, tokens), 0) < counted((tokens, tokens), 1)
    slot = jnp.dot(
        named.astype(F32).astype(BF16),
        earlier.astype(F32).astype(BF16),
        preferred_element_type=F32,
    ).astype(jnp.int32)
    grad = grad_ref[...]
    total = jnp.zeros((rows, 128), F32)
    for part in range(PARTS):
        hit = named & (slot == row + (0, 8, 16, 12)[part])
        if part == 2:
            hit = hit & (row < 4)
        if part == 3:
            hit = hit & (row >= 4)
        pick_ref[part] = hit.astype(F32).astype(BF16)
        mine = times_t(jnp.where(hit, weight, 0.0).astype(BF16), grad).astype(BF16)
        total = total + jnp.dot(mine, placing(part, width), preferred_element_type=F32)
    tile = total.astype(BF16)
    for k in range(copies):
        tile_ref[k] = tile


def unpack_kernel(width, got_ref, out_ref):
    nb, na, rows, _ = got_ref.shape
    short = rows // 2
    at, source = counted((rows, rows), 0), counted((rows, rows), 1)
    number = at & (short - 1)
    wanted = (number >> 2) * 8 + (number & 3) + jnp.where(at >= short, 4, 0)
    halves = (source == wanted).astype(F32).astype(BF16)
    whole, upper, lower = [], [], []
    for a in range(na):
        for b in range(nb):
            tile = got_ref[b, a]
            whole.append(tile[:, :width])
            upper.append(tile[:, width : 2 * width])
            rest = jnp.dot(halves, tile, preferred_element_type=F32).astype(BF16)
            lower.append(rest[:short, 2 * width : 2 * width + width // 2])
            lower.append(rest[short:, 2 * width : 2 * width + width // 2])
    out_ref[:rows, :] = jnp.concatenate(whole, axis=1)
    out_ref[rows : 2 * rows, :] = jnp.concatenate(upper, axis=1)
    out_ref[2 * rows :, :] = jnp.concatenate(lower, axis=1)


def pack_kernel(width, in_ref, out_ref):
    nb, na, rows, _ = out_ref.shape
    peers = in_ref.shape[0]
    short = rows // 2
    total = in_ref[0].astype(F32)
    for k in range(1, peers):
        total = total + in_ref[k].astype(F32)
    total = total.astype(BF16)
    at, source = counted((rows, short), 0), counted((rows, short), 1)
    wanted = (at >> 3) * 4 + (at & 3)
    low = ((source == wanted) & ((at & 7) < 4)).astype(F32).astype(BF16)
    high = ((source == wanted) & ((at & 7) >= 4)).astype(F32).astype(BF16)
    lows = jnp.dot(low, total[2 * rows :], preferred_element_type=F32).astype(BF16)
    highs = jnp.dot(high, total[2 * rows :], preferred_element_type=F32).astype(BF16)
    blank = jnp.zeros((rows, 128 - 2 * width - width // 2), BF16)
    for a in range(na):
        for b in range(nb):
            at = (a * nb + b) * width
            half = lows[:, at : at + width // 2] + highs[:, at + width // 2 : at + width]
            out_ref[b, a] = jnp.concatenate(
                [total[:rows, at : at + width], total[rows : 2 * rows, at : at + width], half, blank],
                axis=1,
            )


def final_kernel(got_ref, pick_ref, out_ref):
    width = out_ref.shape[0]
    total = got_ref[0].astype(F32)
    for k in range(1, got_ref.shape[0]):
        total = total + got_ref[k].astype(F32)
    total = total.astype(BF16)
    out = jnp.zeros(out_ref.shape, F32)
    for part in range(PARTS):
        rows = times_t(placing(part, width), total).astype(BF16)
        out = out + jnp.dot(rows, pick_ref[part], preferred_element_type=F32)
    out_ref[...] = out.astype(BF16)


def weights_kernel(cap, core_ref, down_ref, saved_ref, down_out, pre_out, turned):
    nx, nz, width, _ = down_out.shape
    features = nx * nz * width
    for at in range(0, features, 128):
        to = min(at + 128, features)
        turned[at:to, :] = down_ref[:, at:to].T
    for z in range(nz):
        for x in range(nx):
            at = (z * nx + x) * width
            down_out[x, z] = turned[at : at + width, :]
    slots = saved_ref.shape[1]
    half = slots // 2
    eight = half // cap * 8
    row, source = counted((half, slots), 0), counted((half, slots), 1)
    rest = row - 2 * eight
    block = jnp.where(row < 2 * eight, (row & (eight - 1)) >> 3, rest >> 2)
    slot = jnp.where(row < eight, row & 7, jnp.where(row < 2 * eight, 8 + (row & 7), 16 + (rest & 3)))
    for other in range(2):
        core = core_ref[0] if other == 0 else 1 - core_ref[0]
        picks = (source == (block * 2 + core) * cap + slot).astype(F32).astype(BF16)
        for kind in range(2):
            mine = jnp.dot(picks, saved_ref[kind], preferred_element_type=F32)
            pre_out[other, kind] = mine.astype(BF16)


def through_kernel(other, rows_ref, down_ref, both_ref, pre_ref, out_ref):
    nx = rows_ref.shape[0]
    projected = jnp.dot(rows_ref[0], down_ref[0], preferred_element_type=F32)
    for k in range(1, nx):
        projected = projected + jnp.dot(rows_ref[k], down_ref[k], preferred_element_type=F32)
    gate_pre = pre_ref[other, 0].astype(F32)
    up_pre = pre_ref[other, 1].astype(F32)
    sig = jax.nn.sigmoid(gate_pre)
    gate_grad = (projected * up_pre * sig * (1.0 + gate_pre * (1.0 - sig))).astype(BF16)
    up_grad = (projected * gate_pre * sig).astype(BF16)
    both = jnp.concatenate([gate_grad, up_grad], axis=1)
    for k in range(nx):
        weights = both_ref[:, k].reshape(out_ref.shape[2], both.shape[1])
        out_ref[k] = times_t(both, weights).astype(out_ref.dtype)


def call(kernel, name, out, *args, dtype=BF16, scratch=(), flops=4000000, grant=8):
    shapes = [jax.ShapeDtypeStruct(s, dtype) for s in out]
    whole = pl.BlockSpec(memory_space=pltpu.VMEM)
    scalars = pl.BlockSpec(memory_space=pltpu.SMEM)
    return pl.pallas_call(
        kernel,
        name=name,
        out_shape=shapes,
        in_specs=[scalars if a.ndim == 1 else whole for a in args],
        out_specs=[whole] * len(out),
        scratch_shapes=scratch,
        compiler_params=pltpu.CompilerParams(vmem_limit_bytes=grant << 20),
        cost_estimate=pl.CostEstimate(flops=flops, bytes_accessed=300000, transcendentals=0),
    )(*args)


def local(out_grad, gate_probs, expert_ids, saved_gate, saved_up, w_gate, w_up, w_down):
    na, nb, nx, ny, nh, nc = (lax.axis_size(a) for a in ("za", "zb", "x", "y", "zh", "c"))
    experts = ny * nh
    tokens, width = out_grad.shape
    slots = saved_gate.shape[1]
    cap = slots // (experts * nc)
    half = experts * cap
    hid = w_down.shape[1]
    span = na * nb * width
    rows = experts * 8
    assert cap == 20 and 2 * width + width // 2 <= 128

    sent, picks = call(
        dispatch_kernel,
        "dispatch",
        [(na, rows, 128), (PARTS, rows, tokens)],
        expert_ids.T,
        gate_probs.T,
        out_grad.T,
        grant=60,
    )
    sent, w_down, w_gate, w_up, saved_gate, saved_up = lax.optimization_barrier(
        (sent, w_down, w_gate, w_up, saved_gate, saved_up)
    )

    features = nx * span
    nz = na * nb
    both = jnp.concatenate([w_gate[0], w_up[0]], axis=1).reshape(nz, nx, width, 2 * hid)
    down, pre = call(
        functools.partial(weights_kernel, cap),
        "weights",
        [(nx, nz, width, hid), (2, 2, half, hid)],
        lax.axis_index("c").astype(jnp.int32).reshape(1),
        w_down[0],
        jnp.concatenate([saved_gate, saved_up]),
        scratch=[pltpu.VMEM((features, hid), BF16)],
        flops=100000000,
    )
    down = down.reshape(nx, span, hid)
    got = exchange(sent.reshape(na * experts, 8, 128), FAR)
    got, down, both, pre = lax.optimization_barrier((got, down, both, pre))
    got = jnp.broadcast_to(got.reshape(1, na * rows, 128), (nb, na * rows, 128))
    got = exchange(got, "zb").reshape(nb, na, rows, 128)
    (got,) = call(functools.partial(unpack_kernel, width), "unpack", [(half, span)], got)
    own_rows = lax.all_gather(got, "x")
    other_rows = swap(own_rows)

    def through(rows, other, dtype):
        (out,) = call(
            functools.partial(through_kernel, other),
            ("own", "other")[other],
            [(nx, half, span)],
            rows,
            down,
            both,
            pre,
            dtype=dtype,
            flops=2 * half * features * hid * 3,
        )
        return out

    for_own = through(own_rows, 0, F32)
    for_other = through(other_rows, 1, BF16)
    shares = (for_own + swap(for_other).astype(F32)).astype(BF16)
    shares = exchange(shares, "x")
    (back,) = call(functools.partial(pack_kernel, width), "pack", [(nb, na, rows, 128)], shares)
    back = exchange(back.reshape(nb, na * rows, 128), "zb")
    back = jnp.sum(back.astype(F32), axis=0).astype(BF16)
    back = exchange(back.reshape(na * experts, 8, 128), FAR).reshape(na, rows, 128)
    (out,) = call(final_kernel, "pick", [(width, tokens)], back, picks)
    return out.T


def solution(mesh):
    split = Mesh(mesh.devices.reshape(4, 4, 4, 4, 2, 2), ("za", "zb", "x", "y", "zh", "c"))
    return jax.shard_map(
        local,
        mesh=split,
        in_specs=(
            P(EXPERT, DP),
            P(EXPERT, None),
            P(EXPERT, None),
            P(EXPERT, None, DP),
            P(EXPERT, None, DP),
            P(EXPERT, None, DP),
            P(EXPERT, None, DP),
            P(EXPERT, DP, None),
        ),
        out_specs=P(EXPERT, DP),
        check_vma=False,
    )
```

```python
import functools

import jax
import jax.numpy as jnp
from jax import lax
from jax.experimental import pallas as pl
from jax.experimental.pallas import tpu as pltpu
from jax.sharding import Mesh
from jax.sharding import PartitionSpec as P

EXPERT = ("y", "zh", "c")
DP = ("za", "zb", "x")
FAR = ("za", "y", "zh")
F32 = jnp.float32
BF16 = jnp.bfloat16


def exchange(tiles, axes):
    return lax.all_to_all(tiles, axes, split_axis=0, concat_axis=0, tiled=True)


def swap(value):
    return lax.ppermute(value, "c", [(0, 1), (1, 0)])


def times_t(a, b):
    return lax.dot_general(a, b, (((1,), (1,)), ((), ())), preferred_element_type=F32)


PARTS = 4


def counted(shape, dim):
    return lax.broadcasted_iota(jnp.int32, shape, dim)


def placing(part, width):
    feature, lane = counted((width, 128), 0), counted((width, 128), 1)
    if part < 2:
        hit = lane == feature + part * width
    elif part == 2:
        hit = (lane == feature + 2 * width) & (feature < width // 2)
    else:
        hit = (lane == feature + 2 * width - width // 2) & (feature >= width // 2)
    return hit.astype(F32).astype(BF16)


def dispatch_kernel(ids_ref, prob_ref, grad_ref, tile_ref, pick_ref):
    copies, rows, _ = tile_ref.shape
    width, tokens = grad_ref.shape
    expert = counted((rows, tokens), 0) >> 3
    row = counted((rows, tokens), 0) & 7
    first = ids_ref[0:1, :] == expert
    second = ids_ref[1:2, :] == expert
    named = first | second
    prob = prob_ref[...].astype(F32)
    weight = jnp.where(first, prob[0:1, :], 0.0) + jnp.where(second, prob[1:2, :], 0.0)
    earlier = counted((tokens, tokens), 0) < counted((tokens, tokens), 1)
    slot = jnp.dot(
        named.astype(F32).astype(BF16),
        earlier.astype(F32).astype(BF16),
        preferred_element_type=F32,
    ).astype(jnp.int32)
    grad = grad_ref[...]
    total = jnp.zeros((rows, 128), F32)
    for part in range(PARTS):
        hit = named & (slot == row + (0, 8, 16, 12)[part])
        if part == 2:
            hit = hit & (row < 4)
        if part == 3:
            hit = hit & (row >= 4)
        pick_ref[part] = hit.astype(F32).astype(BF16)
        mine = times_t(jnp.where(hit, weight, 0.0).astype(BF16), grad).astype(BF16)
        total = total + jnp.dot(mine, placing(part, width), preferred_element_type=F32)
    tile = total.astype(BF16)
    for k in range(copies):
        tile_ref[k] = tile


def unpack_kernel(width, got_ref, out_ref):
    nb, na, rows, _ = got_ref.shape
    short = rows // 2
    at, source = counted((rows, rows), 0), counted((rows, rows), 1)
    number = at & (short - 1)
    wanted = (number >> 2) * 8 + (number & 3) + jnp.where(at >= short, 4, 0)
    halves = (source == wanted).astype(F32).astype(BF16)
    whole, upper, lower = [], [], []
    for a in range(na):
        for b in range(nb):
            tile = got_ref[b, a]
            whole.append(tile[:, :width])
            upper.append(tile[:, width : 2 * width])
            rest = jnp.dot(halves, tile, preferred_element_type=F32).astype(BF16)
            lower.append(rest[:short, 2 * width : 2 * width + width // 2])
            lower.append(rest[short:, 2 * width : 2 * width + width // 2])
    out_ref[:rows, :] = jnp.concatenate(whole, axis=1)
    out_ref[rows : 2 * rows, :] = jnp.concatenate(upper, axis=1)
    out_ref[2 * rows :, :] = jnp.concatenate(lower, axis=1)


def pack_kernel(width, in_ref, out_ref):
    nb, na, rows, _ = out_ref.shape
    peers = in_ref.shape[0]
    short = rows // 2
    total = in_ref[0].astype(F32)
    for k in range(1, peers):
        total = total + in_ref[k].astype(F32)
    total = total.astype(BF16)
    at, source = counted((rows, short), 0), counted((rows, short), 1)
    wanted = (at >> 3) * 4 + (at & 3)
    low = ((source == wanted) & ((at & 7) < 4)).astype(F32).astype(BF16)
    high = ((source == wanted) & ((at & 7) >= 4)).astype(F32).astype(BF16)
    lows = jnp.dot(low, total[2 * rows :], preferred_element_type=F32).astype(BF16)
    highs = jnp.dot(high, total[2 * rows :], preferred_element_type=F32).astype(BF16)
    blank = jnp.zeros((rows, 128 - 2 * width - width // 2), BF16)
    for a in range(na):
        for b in range(nb):
            at = (a * nb + b) * width
            half = lows[:, at : at + width // 2] + highs[:, at + width // 2 : at + width]
            out_ref[b, a] = jnp.concatenate(
                [total[:rows, at : at + width], total[rows : 2 * rows, at : at + width], half, blank],
                axis=1,
            )


def final_kernel(got_ref, pick_ref, out_ref):
    width = out_ref.shape[0]
    total = got_ref[0].astype(F32)
    for k in range(1, got_ref.shape[0]):
        total = total + got_ref[k].astype(F32)
    total = total.astype(BF16)
    out = jnp.zeros(out_ref.shape, F32)
    for part in range(PARTS):
        rows = times_t(placing(part, width), total).astype(BF16)
        out = out + jnp.dot(rows, pick_ref[part], preferred_element_type=F32)
    out_ref[...] = out.astype(BF16)


def weights_kernel(
    cap, core_ref, down_ref, gate_ref, up_ref, saved_ref, down_out, both_out, pre_out, turned, block
):
    nx, nz, width, _ = down_out.shape
    features = nx * nz * width
    for at in range(0, features, 128):
        to = min(at + 128, features)
        turned[at:to, :] = down_ref[:, at:to].T
    for z in range(nz):
        for x in range(nx):
            at = (z * nx + x) * width
            down_out[x, z] = turned[at : at + width, :]
    span, hid = nz * width, both_out.shape[1] // 2
    for kind, ref in enumerate((gate_ref, up_ref)):
        for x in range(nx):
            for z in range(nz):
                at = (z * nx + x) * width
                block[z * width : (z + 1) * width, :] = ref[at : at + width, :]
            for at in range(0, span, 128):
                to = min(at + 128, span)
                both_out[x, kind * hid : (kind + 1) * hid, at:to] = block[at:to, :].T
    slots = saved_ref.shape[1]
    half = slots // 2
    eight = half // cap * 8
    row, source = counted((half, slots), 0), counted((half, slots), 1)
    rest = row - 2 * eight
    block = jnp.where(row < 2 * eight, (row & (eight - 1)) >> 3, rest >> 2)
    slot = jnp.where(row < eight, row & 7, jnp.where(row < 2 * eight, 8 + (row & 7), 16 + (rest & 3)))
    for other in range(2):
        core = core_ref[0] if other == 0 else 1 - core_ref[0]
        picks = (source == (block * 2 + core) * cap + slot).astype(F32).astype(BF16)
        for kind in range(2):
            mine = jnp.dot(picks, saved_ref[kind], preferred_element_type=F32)
            pre_out[other, kind] = mine.astype(BF16)


def through_kernel(other, rows_ref, down_ref, both_ref, pre_ref, out_ref):
    nx = rows_ref.shape[0]
    projected = jnp.dot(rows_ref[0], down_ref[0], preferred_element_type=F32)
    for k in range(1, nx):
        projected = projected + jnp.dot(rows_ref[k], down_ref[k], preferred_element_type=F32)
    gate_pre = pre_ref[other, 0].astype(F32)
    up_pre = pre_ref[other, 1].astype(F32)
    sig = jax.nn.sigmoid(gate_pre)
    gate_grad = (projected * up_pre * sig * (1.0 + gate_pre * (1.0 - sig))).astype(BF16)
    up_grad = (projected * gate_pre * sig).astype(BF16)
    both = jnp.concatenate([gate_grad, up_grad], axis=1)
    for k in range(nx):
        share = jnp.dot(both, both_ref[k], preferred_element_type=F32)
        out_ref[k] = share.astype(out_ref.dtype)


def call(kernel, name, out, *args, dtype=BF16, scratch=(), flops=4000000, grant=8):
    shapes = [jax.ShapeDtypeStruct(s, dtype) for s in out]
    whole = pl.BlockSpec(memory_space=pltpu.VMEM)
    scalars = pl.BlockSpec(memory_space=pltpu.SMEM)
    return pl.pallas_call(
        kernel,
        name=name,
        out_shape=shapes,
        in_specs=[scalars if a.ndim == 1 else whole for a in args],
        out_specs=[whole] * len(out),
        scratch_shapes=scratch,
        compiler_params=pltpu.CompilerParams(vmem_limit_bytes=grant << 20),
        cost_estimate=pl.CostEstimate(flops=flops, bytes_accessed=300000, transcendentals=0),
    )(*args)


def local(out_grad, gate_probs, expert_ids, saved_gate, saved_up, w_gate, w_up, w_down):
    na, nb, nx, ny, nh, nc = (lax.axis_size(a) for a in ("za", "zb", "x", "y", "zh", "c"))
    experts = ny * nh
    tokens, width = out_grad.shape
    slots = saved_gate.shape[1]
    cap = slots // (experts * nc)
    half = experts * cap
    hid = w_down.shape[1]
    span = na * nb * width
    rows = experts * 8
    assert cap == 20 and 2 * width + width // 2 <= 128

    sent, picks = call(
        dispatch_kernel,
        "dispatch",
        [(na, rows, 128), (PARTS, rows, tokens)],
        expert_ids.T,
        gate_probs.T,
        out_grad.T,
        grant=60,
    )
    sent, w_down, w_gate, w_up, saved_gate, saved_up = lax.optimization_barrier(
        (sent, w_down, w_gate, w_up, saved_gate, saved_up)
    )

    features = nx * span
    nz = na * nb
    down, both, pre = call(
        functools.partial(weights_kernel, cap),
        "weights",
        [(nx, nz, width, hid), (nx, 2 * hid, span), (2, 2, half, hid)],
        lax.axis_index("c").astype(jnp.int32).reshape(1),
        w_down[0],
        w_gate[0],
        w_up[0],
        jnp.concatenate([saved_gate, saved_up]),
        scratch=[pltpu.VMEM((features, hid), BF16), pltpu.VMEM((span, hid), BF16)],
        flops=100000000,
    )
    down = down.reshape(nx, span, hid)
    got = exchange(sent.reshape(na * experts, 8, 128), FAR)
    got, down, both, pre = lax.optimization_barrier((got, down, both, pre))
    got = jnp.broadcast_to(got.reshape(1, na * rows, 128), (nb, na * rows, 128))
    got = exchange(got, "zb").reshape(nb, na, rows, 128)
    (got,) = call(functools.partial(unpack_kernel, width), "unpack", [(half, span)], got)
    own_rows = lax.all_gather(got, "x")
    other_rows = swap(own_rows)

    def through(rows, other, dtype):
        (out,) = call(
            functools.partial(through_kernel, other),
            ("own", "other")[other],
            [(nx, half, span)],
            rows,
            down,
            both,
            pre,
            dtype=dtype,
            flops=2 * half * features * hid * 3,
        )
        return out

    for_own = through(own_rows, 0, F32)
    for_other = through(other_rows, 1, BF16)
    shares = (for_own + swap(for_other).astype(F32)).astype(BF16)
    shares = exchange(shares, "x")
    (back,) = call(functools.partial(pack_kernel, width), "pack", [(nb, na, rows, 128)], shares)
    back = exchange(back.reshape(nb, na * rows, 128), "zb")
    back = jnp.sum(back.astype(F32), axis=0).astype(BF16)
    back = exchange(back.reshape(na * experts, 8, 128), FAR).reshape(na, rows, 128)
    (out,) = call(final_kernel, "pick", [(width, tokens)], back, picks)
    return out.T


def solution(mesh):
    split = Mesh(mesh.devices.reshape(4, 4, 4, 4, 2, 2), ("za", "zb", "x", "y", "zh", "c"))
    return jax.shard_map(
        local,
        mesh=split,
        in_specs=(
            P(EXPERT, DP),
            P(EXPERT, None),
            P(EXPERT, None),
            P(EXPERT, None, DP),
            P(EXPERT, None, DP),
            P(EXPERT, None, DP),
            P(EXPERT, None, DP),
            P(EXPERT, DP, None),
        ),
        out_specs=P(EXPERT, DP),
        check_vma=False,
    )
```

```python
import functools

import jax
import jax.numpy as jnp
from jax import lax
from jax.experimental import pallas as pl
from jax.experimental.pallas import tpu as pltpu
from jax.sharding import Mesh
from jax.sharding import PartitionSpec as P

EXPERT = ("y", "zh", "c")
DP = ("za", "zb", "x")
FAR = ("za", "y", "zh")
F32 = jnp.float32
BF16 = jnp.bfloat16


def exchange(tiles, axes):
    return lax.all_to_all(tiles, axes, split_axis=0, concat_axis=0, tiled=True)


def swap(value):
    return lax.ppermute(value, "c", [(0, 1), (1, 0)])


def times_t(a, b):
    return lax.dot_general(a, b, (((1,), (1,)), ((), ())), preferred_element_type=F32)


PARTS = 4


def counted(shape, dim):
    return lax.broadcasted_iota(jnp.int32, shape, dim)


def placing(part, width):
    feature, lane = counted((width, 128), 0), counted((width, 128), 1)
    if part < 2:
        hit = lane == feature + part * width
    elif part == 2:
        hit = (lane == feature + 2 * width) & (feature < width // 2)
    else:
        hit = (lane == feature + 2 * width - width // 2) & (feature >= width // 2)
    return hit.astype(F32).astype(BF16)


def dispatch_kernel(ids_ref, prob_ref, grad_ref, tile_ref, pick_ref):
    copies, rows, _ = tile_ref.shape
    width, tokens = grad_ref.shape
    expert = counted((rows, tokens), 0) >> 3
    row = counted((rows, tokens), 0) & 7
    first = ids_ref[0:1, :] == expert
    second = ids_ref[1:2, :] == expert
    named = first | second
    prob = prob_ref[...].astype(F32)
    weight = jnp.where(first, prob[0:1, :], 0.0) + jnp.where(second, prob[1:2, :], 0.0)
    earlier = counted((tokens, tokens), 0) < counted((tokens, tokens), 1)
    slot = jnp.dot(
        named.astype(F32).astype(BF16),
        earlier.astype(F32).astype(BF16),
        preferred_element_type=F32,
    ).astype(jnp.int32)
    grad = grad_ref[...]
    total = jnp.zeros((rows, 128), F32)
    for part in range(PARTS):
        hit = named & (slot == row + (0, 8, 16, 12)[part])
        if part == 2:
            hit = hit & (row < 4)
        if part == 3:
            hit = hit & (row >= 4)
        pick_ref[part] = hit.astype(F32).astype(BF16)
        mine = times_t(jnp.where(hit, weight, 0.0).astype(BF16), grad).astype(BF16)
        total = total + jnp.dot(mine, placing(part, width), preferred_element_type=F32)
    tile = total.astype(BF16)
    for k in range(copies):
        tile_ref[k] = tile


def unpack_kernel(width, got_ref, out_ref):
    nb, na, rows, _ = got_ref.shape
    short = rows // 2
    at, source = counted((rows, rows), 0), counted((rows, rows), 1)
    number = at & (short - 1)
    wanted = (number >> 2) * 8 + (number & 3) + jnp.where(at >= short, 4, 0)
    halves = (source == wanted).astype(F32).astype(BF16)
    whole, upper, lower = [], [], []
    for a in range(na):
        for b in range(nb):
            tile = got_ref[b, a]
            whole.append(tile[:, :width])
            upper.append(tile[:, width : 2 * width])
            rest = jnp.dot(halves, tile, preferred_element_type=F32).astype(BF16)
            lower.append(rest[:short, 2 * width : 2 * width + width // 2])
            lower.append(rest[short:, 2 * width : 2 * width + width // 2])
    out_ref[:rows, :] = jnp.concatenate(whole, axis=1)
    out_ref[rows : 2 * rows, :] = jnp.concatenate(upper, axis=1)
    out_ref[2 * rows :, :] = jnp.concatenate(lower, axis=1)


def pack_kernel(width, in_ref, out_ref):
    nb, na, rows, _ = out_ref.shape
    peers = in_ref.shape[0]
    short = rows // 2
    total = in_ref[0].astype(F32)
    for k in range(1, peers):
        total = total + in_ref[k].astype(F32)
    total = total.astype(BF16)
    at, source = counted((rows, short), 0), counted((rows, short), 1)
    wanted = (at >> 3) * 4 + (at & 3)
    low = ((source == wanted) & ((at & 7) < 4)).astype(F32).astype(BF16)
    high = ((source == wanted) & ((at & 7) >= 4)).astype(F32).astype(BF16)
    lows = jnp.dot(low, total[2 * rows :], preferred_element_type=F32).astype(BF16)
    highs = jnp.dot(high, total[2 * rows :], preferred_element_type=F32).astype(BF16)
    blank = jnp.zeros((rows, 128 - 2 * width - width // 2), BF16)
    for a in range(na):
        for b in range(nb):
            at = (a * nb + b) * width
            half = lows[:, at : at + width // 2] + highs[:, at + width // 2 : at + width]
            out_ref[b, a] = jnp.concatenate(
                [total[:rows, at : at + width], total[rows : 2 * rows, at : at + width], half, blank],
                axis=1,
            )


def final_kernel(got_ref, pick_ref, out_ref):
    width = out_ref.shape[0]
    total = got_ref[0].astype(F32)
    for k in range(1, got_ref.shape[0]):
        total = total + got_ref[k].astype(F32)
    total = total.astype(BF16)
    out = jnp.zeros(out_ref.shape, F32)
    for part in range(PARTS):
        rows = times_t(placing(part, width), total).astype(BF16)
        out = out + jnp.dot(rows, pick_ref[part], preferred_element_type=F32)
    out_ref[...] = out.astype(BF16)


def weights_kernel(
    cap, core_ref, down_ref, gate_ref, up_ref, saved_ref, down_out, both_out, pre_out, turned, block
):
    nx, nz, width, _ = down_out.shape
    features = nx * nz * width
    for at in range(0, features, 128):
        to = min(at + 128, features)
        turned[at:to, :] = down_ref[:, at:to].T
    for z in range(nz):
        for x in range(nx):
            at = (z * nx + x) * width
            down_out[x, z] = turned[at : at + width, :]
    span, hid = nz * width, both_out.shape[1] // 2
    for kind, ref in enumerate((gate_ref, up_ref)):
        for x in range(nx):
            for z in range(nz):
                at = (z * nx + x) * width
                block[z * width : (z + 1) * width, :] = ref[at : at + width, :]
            for at in range(0, span, 128):
                to = min(at + 128, span)
                both_out[x, kind * hid : (kind + 1) * hid, at:to] = block[at:to, :].T
    slots = saved_ref.shape[1]
    half = slots // 2
    eight = half // cap * 8
    row, source = counted((half, slots), 0), counted((half, slots), 1)
    rest = row - 2 * eight
    block = jnp.where(row < 2 * eight, (row & (eight - 1)) >> 3, rest >> 2)
    slot = jnp.where(row < eight, row & 7, jnp.where(row < 2 * eight, 8 + (row & 7), 16 + (rest & 3)))
    for other in range(2):
        core = core_ref[0] if other == 0 else 1 - core_ref[0]
        picks = (source == (block * 2 + core) * cap + slot).astype(F32).astype(BF16)
        for kind in range(2):
            mine = jnp.dot(picks, saved_ref[kind], preferred_element_type=F32)
            pre_out[other, kind] = mine.astype(BF16)


def through_kernel(other, rows_ref, down_ref, both_ref, pre_ref, out_ref):
    nx = rows_ref.shape[0]
    projected = jnp.dot(rows_ref[0], down_ref[0], preferred_element_type=F32)
    for k in range(1, nx):
        projected = projected + jnp.dot(rows_ref[k], down_ref[k], preferred_element_type=F32)
    gate_pre = pre_ref[other, 0].astype(F32)
    up_pre = pre_ref[other, 1].astype(F32)
    sig = jax.nn.sigmoid(gate_pre)
    gate_grad = (projected * up_pre * sig * (1.0 + gate_pre * (1.0 - sig))).astype(BF16)
    up_grad = (projected * gate_pre * sig).astype(BF16)
    both = jnp.concatenate([gate_grad, up_grad], axis=1)
    for k in range(nx):
        share = jnp.dot(both, both_ref[k], preferred_element_type=F32)
        out_ref[k] = share.astype(out_ref.dtype)


def call(kernel, name, out, *args, dtype=BF16, scratch=(), flops=4000000, grant=8):
    shapes = [jax.ShapeDtypeStruct(s, dtype) for s in out]
    whole = pl.BlockSpec(memory_space=pltpu.VMEM)
    scalars = pl.BlockSpec(memory_space=pltpu.SMEM)
    return pl.pallas_call(
        kernel,
        name=name,
        out_shape=shapes,
        in_specs=[scalars if a.ndim == 1 else whole for a in args],
        out_specs=[whole] * len(out),
        scratch_shapes=scratch,
        compiler_params=pltpu.CompilerParams(vmem_limit_bytes=grant << 20),
        cost_estimate=pl.CostEstimate(flops=flops, bytes_accessed=300000, transcendentals=0),
    )(*args)


def local(out_grad, gate_probs, expert_ids, saved_gate, saved_up, w_gate, w_up, w_down):
    na, nb, nx, ny, nh, nc = (lax.axis_size(a) for a in ("za", "zb", "x", "y", "zh", "c"))
    experts = ny * nh
    tokens, width = out_grad.shape
    slots = saved_gate.shape[1]
    cap = slots // (experts * nc)
    half = experts * cap
    hid = w_down.shape[1]
    span = na * nb * width
    rows = experts * 8
    assert cap == 20 and 2 * width + width // 2 <= 128

    sent, picks = call(
        dispatch_kernel,
        "dispatch",
        [(na, rows, 128), (PARTS, rows, tokens)],
        expert_ids.T,
        gate_probs.T,
        out_grad.T,
        grant=60,
    )
    sent, w_down, w_gate, w_up, saved_gate, saved_up = lax.optimization_barrier(
        (sent, w_down, w_gate, w_up, saved_gate, saved_up)
    )

    features = nx * span
    nz = na * nb
    down, both, pre = call(
        functools.partial(weights_kernel, cap),
        "weights",
        [(nx, nz, width, hid), (nx, 2 * hid, span), (2, 2, half, hid)],
        lax.axis_index("c").astype(jnp.int32).reshape(1),
        w_down[0],
        w_gate[0],
        w_up[0],
        jnp.concatenate([saved_gate, saved_up]),
        scratch=[pltpu.VMEM((features, hid), BF16), pltpu.VMEM((span, hid), BF16)],
        flops=100000000,
    )
    down = down.reshape(nx, span, hid)
    got = exchange(sent.reshape(na * experts, 8, 128), FAR)
    got, down, both, pre = lax.optimization_barrier((got, down, both, pre))
    got = jnp.broadcast_to(got.reshape(1, na * rows, 128), (nb, na * rows, 128))
    got = exchange(got, "zb").reshape(nb, na, rows, 128)
    (got,) = call(functools.partial(unpack_kernel, width), "unpack", [(half, span)], got)
    own_rows = lax.all_gather(got, "x")
    other_rows = swap(own_rows)

    def through(rows, other, dtype):
        (out,) = call(
            functools.partial(through_kernel, other),
            ("own", "other")[other],
            [(nx, half, span)],
            rows,
            down,
            both,
            pre,
            dtype=dtype,
            flops=2 * half * features * hid * 3,
        )
        return out

    for_own = through(own_rows, 0, F32)
    for_other = through(other_rows, 1, BF16)
    shares = (for_own + swap(for_other).astype(F32)).astype(BF16)
    shares = exchange(shares, "x")
    (back,) = call(functools.partial(pack_kernel, width), "pack", [(nb, na, rows, 128)], shares)
    back = exchange(back.reshape(nb, na * rows, 128), "zb")
    back = jnp.sum(back.astype(F32), axis=0).astype(BF16)
    back = back.reshape(na, ny, nh, 8, 128).transpose(2, 0, 1, 3, 4)
    back = exchange(back.reshape(na * experts, 8, 128), ("zh", "za", "y"))
    back = back.reshape(nh, na, ny, 8, 128).transpose(1, 2, 0, 3, 4).reshape(na, rows, 128)
    (out,) = call(final_kernel, "pick", [(width, tokens)], back, picks)
    return out.T


def solution(mesh):
    split = Mesh(mesh.devices.reshape(4, 4, 4, 4, 2, 2), ("za", "zb", "x", "y", "zh", "c"))
    return jax.shard_map(
        local,
        mesh=split,
        in_specs=(
            P(EXPERT, DP),
            P(EXPERT, None),
            P(EXPERT, None),
            P(EXPERT, None, DP),
            P(EXPERT, None, DP),
            P(EXPERT, None, DP),
            P(EXPERT, None, DP),
            P(EXPERT, DP, None),
        ),
        out_specs=P(EXPERT, DP),
        check_vma=False,
    )
```
